64 devices in a mesh: rep: 8 (over x, y, core), dp: 8 (over z).
Axes of the slice: x: 2, y: 2, z: 8, core: 2. Of those that a mesh axis runs over, the one named last changes fastest.
The devices are a block of a 4x4x8 slice.
Arguments:
- x: bfloat16 [64, 4096, 512], P(('rep', 'dp')), parts along dimension 0
- dy: bfloat16 [64, 4096, 512], P(('rep', 'dp')), parts along dimension 0
- w_gate: bfloat16 [2, 512, 1664], replicated
- w_up: bfloat16 [2, 512, 1664], replicated
- w_down: bfloat16 [2, 1664, 512], replicated
- m_w_gate: float32 [2, 512, 1664], P(None, 'dp')
- m_w_up: float32 [2, 512, 1664], P(None, 'dp')
- m_w_down: float32 [2, 1664, 512], P(None, 'dp')
- v_w_gate: float32 [2, 512, 1664], P(None, 'dp')
- v_w_up: float32 [2, 512, 1664], P(None, 'dp')
- v_w_down: float32 [2, 1664, 512], P(None, 'dp')
Outputs:
- output 1: bfloat16 [16, 512, 1664], P('rep'), parts along dimension 0
- output 2: bfloat16 [16, 512, 1664], P('rep'), parts along dimension 0
- output 3: bfloat16 [16, 1664, 512], P('rep'), parts along dimension 0
- output 4: float32 [16, 512, 1664], P('rep', 'dp'), parts along dimension 0
- output 5: float32 [16, 512, 1664], P('rep', 'dp'), parts along dimension 0
- output 6: float32 [16, 1664, 512], P('rep', 'dp'), parts along dimension 0
- output 7: float32 [16, 512, 1664], P('rep', 'dp'), parts along dimension 0
- output 8: float32 [16, 512, 1664], P('rep', 'dp'), parts along dimension 0
- output 9: float32 [16, 1664, 512], P('rep', 'dp'), parts along dimension 0
There are 8 independent parts. The reference program is written for one: setup_inputs(seed, part) draws one part's arguments, and reference() takes and returns one part's arrays. A program takes and returns all parts, laid end to end along the dimension named above; an argument that names none is the same for every part.
All inputs are finite; a program needn't handle non-finite values.
Results may differ from the reference program's by a relative error of at most 0.022.
Values are sent between devices in bfloat16 or wider.
A program may use at most 768 MiB of HBM per device.

```python
import jax
import jax.numpy as jnp
from jax import lax

SEQUENCES = 8
TOKENS = 4096
D = 512
FF = 1664
LAYERS = 2
NAMES = ("w_gate", "w_up", "w_down")
SHAPES = {"w_gate": (LAYERS, D, FF), "w_up": (LAYERS, D, FF), "w_down": (LAYERS, FF, D)}


def bump(key, n, height):
    away = (jnp.arange(n, dtype=jnp.int32) - jax.random.randint(key, (), 0, n, jnp.int32)) % n
    return jnp.where(away < n // 8, height, 1.0)


def together(key, own, strength):
    shared = jax.random.normal(key, own.shape[1:], jnp.float32)
    return (own + strength * shared) * lax.rsqrt(1 + strength * strength)


def setup_inputs(seed: int = 0, part: int = 0) -> dict:
    kx, kdy, ka, kb, kz, kf, kh, kl, *keys = jax.random.split(jax.random.key(seed), 8 + 3 * len(NAMES))
    kx, kdy, ka, kb = (jax.random.fold_in(k, part) for k in (kx, kdy, ka, kb))
    kw, km, kv = (keys[i::3] for i in range(3))
    shape = (SEQUENCES, TOKENS, D)
    much_x, much_dy = jax.random.uniform(kz, (2,), jnp.float32, 0.0, 1.0)
    loud = 2.0 ** jax.random.uniform(jax.random.fold_in(kz, 1), (), jnp.float32, -1.0, 2.0)
    layers = 2.0 ** jax.random.uniform(kl, (LAYERS, 1, 1), jnp.float32, -1.0, 1.0)
    x = together(ka, jax.random.normal(kx, shape, jnp.float32), much_x) * bump(kf, D, 4.0)
    dy = together(kb, jax.random.normal(kdy, shape, jnp.float32), much_dy)
    drawn = {"x": x.astype(jnp.bfloat16), "dy": (loud * dy * (SEQUENCES * TOKENS) ** -0.5).astype(jnp.bfloat16)}
    for key, name in zip(kw, NAMES, strict=True):
        w = jax.random.normal(key, SHAPES[name], jnp.float32) * SHAPES[name][1] ** -0.5
        drawn[name] = (w * {"w_gate": 1.0, "w_up": bump(kh, FF, 4.0), "w_down": layers}[name]).astype(jnp.bfloat16)
    for key, name in zip(km, NAMES, strict=True):
        drawn[f"m_{name}"] = 0.1 * jax.random.normal(key, SHAPES[name], jnp.float32)
    for key, name in zip(kv, NAMES, strict=True):
        drawn[f"v_{name}"] = jax.random.uniform(key, SHAPES[name], jnp.float32, 0.005, 0.015)
    return drawn


def matmul(a, w):
    return jnp.dot(a, w, preferred_element_type=jnp.float32).astype(jnp.bfloat16)


def normed(h):
    wide = h.astype(jnp.float32)
    scale = lax.rsqrt(jnp.mean(wide**2, -1, keepdims=True) + 1e-6)
    return (wide * scale).astype(jnp.bfloat16)


def layer(h, w):
    a = normed(h)
    gate = jnp.dot(a, w["w_gate"], preferred_element_type=jnp.float32)
    up = jnp.dot(a, w["w_up"], preferred_element_type=jnp.float32)
    return h + matmul((jax.nn.silu(gate) * up).astype(jnp.bfloat16), w["w_down"])


def adamw(w, m, v, g):
    m = 0.9 * m + 0.1 * g
    v = 0.95 * v + 0.05 * g * g
    step = m * lax.rsqrt(v + 1e-8) + 0.1 * w
    return (w - 0.02 * step).astype(jnp.bfloat16), m, v


def clipped(gradients, sum_of_squares, count):
    factor = jnp.minimum(1.0, 0.5 * lax.rsqrt(sum_of_squares / count + 1e-30))
    return [g * factor for g in gradients]


def stack(weights, h):
    return lax.scan(lambda h, w: (layer(h, w), None), h, weights)[0]


def reference(x, dy, w_gate, w_up, w_down, m_w_gate, m_w_up, m_w_down, v_w_gate, v_w_up, v_w_down):
    weights = dict(zip(NAMES, (w_gate, w_up, w_down), strict=True))

    def take(so_far, sequence):
        h, by_y = sequence
        _, back = jax.vjp(lambda w: stack(w, h), weights)
        return jax.tree.map(lambda total, term: total + term.astype(jnp.float32), so_far, back(by_y)[0]), None

    none_yet = {name: jnp.zeros(w.shape, jnp.float32) for name, w in weights.items()}
    by_weights, _ = lax.scan(take, none_yet, (x, dy))
    gradients = [by_weights[name].astype(jnp.bfloat16).astype(jnp.float32) for name in NAMES]
    gradients = clipped(gradients, sum(jnp.sum(g * g) for g in gradients), sum(g.size for g in gradients))
    new = [
        adamw(w.astype(jnp.float32), m, v, g)
        for w, m, v, g in zip((w_gate, w_up, w_down), (m_w_gate, m_w_up, m_w_down), (v_w_gate, v_w_up, v_w_down), gradients, strict=True)
    ]
    return tuple(one[which] for which in range(3) for one in new)
```

```python
import functools

import jax
import jax.numpy as jnp
from jax import lax
from jax.experimental import pallas as pl
from jax.experimental.pallas import tpu as pltpu
from jax.sharding import PartitionSpec as P

F32, BF16 = jnp.float32, jnp.bfloat16
MESH = pl.DeviceIdType.MESH
TILE = 256
VMEM_LIMIT = 63 * 1024 * 1024


def dot(a, b, dims):
    return lax.dot_general(a, b, (dims, ((), ())), preferred_element_type=F32)


NN, NT, TN = ((1,), (0,)), ((1,), (1,)), ((0,), (0,))


def scale_of(wide):
    return lax.rsqrt(jnp.mean(wide * wide, -1, keepdims=True) + 1e-6)


def first_kernel(x_ref, dy_ref, wg_ref, wu_ref, wd_ref, gate_ref, up_ref, h_ref, dg_ref, du_ref, og_ref, ou_ref, od_ref, ag_ref, au_ref, ad_ref):
    step, last = pl.program_id(0), pl.num_programs(0) - 1

    @pl.when(step == 0)
    def _():
        for ref in (ag_ref, au_ref, ad_ref):
            ref[...] = jnp.zeros_like(ref)

    x = x_ref[...]
    wide = x.astype(F32)
    a = (wide * scale_of(wide)).astype(BF16)
    gate = dot(a, wg_ref[0], NN)
    up = dot(a, wu_ref[0], NN)
    gate_ref[...] = gate
    up_ref[...] = up
    act = (gate * jax.nn.sigmoid(gate) * up).astype(BF16)
    h = x + dot(act, wd_ref[0], NN).astype(BF16)
    h_ref[...] = h
    wide = h.astype(F32)
    a = (wide * scale_of(wide)).astype(BF16)
    dy = dy_ref[...]
    dact = dot(dy, wd_ref[1], NT).astype(BF16).astype(F32)
    gate = dot(a, wg_ref[1], NN)
    up = dot(a, wu_ref[1], NN)
    s = jax.nn.sigmoid(gate)
    silu = gate * s
    act = (silu * up).astype(BF16)
    dg = (dact * up * (s * (1.0 + gate * (1.0 - s)))).astype(BF16)
    du = (dact * silu).astype(BF16)
    dg_ref[...] = dg
    du_ref[...] = du
    ad_ref[...] += dot(act, dy, TN)
    ag_ref[...] += dot(a, dg, TN)
    au_ref[...] += dot(a, du, TN)

    @pl.when(step == last)
    def _():
        og_ref[...] = ag_ref[...].astype(BF16)
        ou_ref[...] = au_ref[...].astype(BF16)
        od_ref[...] = ad_ref[...].astype(BF16)


def second_kernel(x_ref, dy_ref, wg_ref, wu_ref, wd_ref, gate_ref, up_ref, h_ref, dg_ref, du_ref, og_ref, ou_ref, od_ref, ag_ref, au_ref, ad_ref):
    step, last = pl.program_id(0), pl.num_programs(0) - 1

    @pl.when(step == 0)
    def _():
        for ref in (ag_ref, au_ref, ad_ref):
            ref[...] = jnp.zeros_like(ref)

    da = dot(dg_ref[...], wg_ref[0], NT).astype(BF16) + dot(du_ref[...], wu_ref[0], NT).astype(BF16)
    da = da.astype(F32)
    wide = h_ref[...].astype(F32)
    scale = scale_of(wide)
    inner = jnp.mean(da * wide, -1, keepdims=True)
    dh = dy_ref[...] + (scale * da - wide * (scale * scale * scale * inner)).astype(BF16)
    dact = dot(dh, wd_ref[0], NT).astype(BF16).astype(F32)
    gate, up = gate_ref[...], up_ref[...]
    s = jax.nn.sigmoid(gate)
    silu = gate * s
    act = (silu * up).astype(BF16)
    dg = (dact * up * (s * (1.0 + gate * (1.0 - s)))).astype(BF16)
    du = (dact * silu).astype(BF16)
    wide = x_ref[...].astype(F32)
    a = (wide * scale_of(wide)).astype(BF16)
    ad_ref[...] += dot(act, dh, TN)
    ag_ref[...] += dot(a, dg, TN)
    au_ref[...] += dot(a, du, TN)

    @pl.when(step == last)
    def _():
        og_ref[...] = ag_ref[...].astype(BF16)
        ou_ref[...] = au_ref[...].astype(BF16)
        od_ref[...] = ad_ref[...].astype(BF16)


def chains_of(layers, shapes, n):
    chains = []
    for layer in layers:
        for k, (rows, _) in enumerate(shapes):
            block = rows // n
            cut = -(-(block // 2) // 16) * 16
            if layer % 2:
                cut = block - cut
            chains.append((layer, k, 0, block, 0, cut))
            chains.append((layer, k, 1, block, cut, block - cut))
    return chains


def tail_kernel(
    n, count, chains,
    t00, t01, t02, t10, t11, t12, w0, w1, w2, m0, m1, m2, v0, v1, v2,
    o0, o1, o2, om0, om1, om2, ov0, ov1, ov2,
    wide_recv, tall_recv, g0, g1, g2, wb0, wb1, wb2, part, parts, send_sem, recv_sem, gsend_sem, grecv_sem, psend_sem, precv_sem, local_sem,
):
    me = lax.axis_index("dp")
    terms, w, m, v = ((t00, t01, t02), (t10, t11, t12)), (w0, w1, w2), (m0, m1, m2), (v0, v1, v2)
    out, om, ov, g, wb = (o0, o1, o2), (om0, om1, om2), (ov0, ov1, ov2), (g0, g1, g2), (wb0, wb1, wb2)
    fetches = []
    for k in range(3):
        block = wb[k].shape[1]
        fetches.append(pltpu.make_async_copy(w[k].at[:, pl.ds(pl.multiple_of(me * block, 16), block), :], wb[k], local_sem.at[k]))
    for f in fetches:
        f.start()

    barrier = pltpu.get_barrier_semaphore()
    for d in range(1, n):
        pl.semaphore_signal(barrier, inc=1, device_id={"dp": lax.rem(me + d, n)}, device_id_type=MESH)
    pl.semaphore_wait(barrier, n - 1)

    def peer(way):
        return {"dp": lax.rem(me + (1 if way == 0 else n - 1), n)}

    def rows(chain, owner):
        _, _, _, block, off, size = chain
        return pl.ds(pl.multiple_of(owner * block + off, 16), size)

    def owner(way, s):
        return lax.rem(me + (2 * n - 1 - s if way == 0 else 1 + s), n)

    def slot(i, s):
        _, k, _, _, _, size = chains[i]
        return (wide_recv if k < 2 else tall_recv).at[index[i], s, pl.ds(0, size)]

    index, seen = [], [0, 0]
    for c in chains:
        kind = 0 if c[1] < 2 else 1
        index.append(seen[kind])
        seen[kind] += 1

    def copy(i, src, s):
        return pltpu.make_async_remote_copy(
            src_ref=src, dst_ref=slot(i, s), send_sem=send_sem.at[i, s], recv_sem=recv_sem.at[i, s],
            device_id=peer(chains[i][2]), device_id_type=MESH,
        )

    def term(i, which):
        c = chains[i]
        return terms[c[0]][c[1]].at[rows(c, which), :]

    for i, c in enumerate(chains):
        copy(i, term(i, owner(c[2], 0)), 0).start()

    def hop(s, _):
        for i, c in enumerate(chains):
            copy(i, slot(i, s), s).wait_recv()
            total = slot(i, s)[...].astype(F32) + term(i, owner(c[2], s + 1))[...].astype(F32)
            slot(i, s)[...] = total.astype(BF16)
            copy(i, slot(i, s), s + 1).start()
        return 0

    lax.fori_loop(0, n - 2, hop, 0)
    squares = jnp.zeros((), F32)
    for i, c in enumerate(chains):
        layer, k, way, block, off, size = c
        copy(i, slot(i, n - 2), n - 2).wait_recv()
        total = slot(i, n - 2)[...].astype(F32) + term(i, me)[...].astype(F32)
        total = total.astype(BF16)
        g[k][layer, pl.ds(off, size), :] = total
        total = total.astype(F32)
        squares += jnp.sum(total * total)

    part[...] = jnp.full(part.shape, squares, F32)

    def share(d):
        return pltpu.make_async_remote_copy(
            src_ref=part, dst_ref=parts.at[me], send_sem=psend_sem.at[d - 1], recv_sem=precv_sem.at[d - 1],
            device_id={"dp": lax.rem(me + d, n)}, device_id_type=MESH,
        )

    for d in range(1, n):
        share(d).start()
    parts[me] = part[...]
    for f in fetches:
        f.wait()
    for d in range(1, n):
        share(d).wait()
    total = parts[0]
    for d in range(1, n):
        total += parts[d]
    factor = jnp.minimum(1.0, 0.5 * lax.rsqrt(total / count + 1e-30))[0:1, 0:1]

    def spread(i, s, which):
        c = chains[i]
        there = out[c[1]].at[c[0], rows(c, which), :]
        return pltpu.make_async_remote_copy(
            src_ref=there, dst_ref=there, send_sem=gsend_sem.at[i, s], recv_sem=grecv_sem.at[i, s],
            device_id=peer(c[2]), device_id_type=MESH,
        )

    for i, c in enumerate(chains):
        layer, k, way, block, off, size = c
        here = pl.ds(off, size)
        grad = g[k][layer, here, :].astype(F32) * factor
        mm = 0.9 * m[k][layer, here, :] + 0.1 * grad
        vv = 0.95 * v[k][layer, here, :] + 0.05 * grad * grad
        om[k][layer, here, :] = mm
        ov[k][layer, here, :] = vv
        old = wb[k][layer, here, :].astype(F32)
        new = old - 0.02 * (mm * lax.rsqrt(vv + 1e-8) + 0.1 * old)
        out[k][layer, rows(c, me), :] = new.astype(BF16)
        spread(i, 0, me).start()

    def came(way, s):
        return lax.rem(me + (2 * n - 1 - s if way == 0 else 1 + s), n)

    def pass_on(s, _):
        for i, c in enumerate(chains):
            spread(i, s, came(c[2], s)).wait_recv()
            spread(i, s + 1, came(c[2], s)).start()
        return 0

    lax.fori_loop(0, n - 2, pass_on, 0)
    for i, c in enumerate(chains):
        spread(i, n - 2, came(c[2], n - 2)).wait_recv()

    def drain(s, _):
        for i in range(len(chains)):
            copy(i, slot(i, s), s).wait_send()
            spread(i, s, me).wait_send()
        return 0

    lax.fori_loop(0, n - 1, drain, 0)


def on_a_device(n, x, dy, *arrays):
    w, m, v = (arrays[i : i + 3] for i in (0, 3, 6))
    layers, width, hidden = w[0].shape
    x, dy = x.reshape(x.shape[-2:]), dy.reshape(dy.shape[-2:])
    tokens = x.shape[0]

    def tile(cols):
        return pl.BlockSpec((TILE, cols), lambda i: (i, 0))

    def whole(shape, at=None):
        return pl.BlockSpec(shape, lambda i: at or (0,) * len(shape), pipeline_mode=pl.Buffered(1))

    shapes = [(width, hidden), (width, hidden), (hidden, width)]
    flops = 2 * tokens * width * hidden
    grads = [jax.ShapeDtypeStruct(s, BF16) for s in shapes]
    params = pltpu.CompilerParams(dimension_semantics=("arbitrary",), vmem_limit_bytes=VMEM_LIMIT)
    sums = [pltpu.VMEM(s, F32) for s in shapes]
    gate, up, h, dg, du, *late = pl.pallas_call(
        first_kernel,
        grid=(tokens // TILE,),
        in_specs=[tile(width), tile(width), *(whole(t.shape) for t in w)],
        out_specs=[tile(hidden), tile(hidden), tile(width), tile(hidden), tile(hidden), *(whole(s) for s in shapes)],
        out_shape=[
            jax.ShapeDtypeStruct((tokens, hidden), F32), jax.ShapeDtypeStruct((tokens, hidden), F32),
            jax.ShapeDtypeStruct((tokens, width), BF16),
            jax.ShapeDtypeStruct((tokens, hidden), BF16), jax.ShapeDtypeStruct((tokens, hidden), BF16), *grads,
        ],
        scratch_shapes=sums,
        compiler_params=params,
        cost_estimate=pl.CostEstimate(flops=9 * flops, bytes_accessed=16 * tokens * hidden, transcendentals=0),
        name="first",
    )(x, dy, *w)

    early = pl.pallas_call(
        second_kernel,
        grid=(tokens // TILE,),
        in_specs=[
            tile(width), tile(width), whole((1, width, hidden), (1, 0, 0)), whole((1, width, hidden), (1, 0, 0)),
            whole((1, hidden, width)), tile(hidden), tile(hidden), tile(width), tile(hidden), tile(hidden),
        ],
        out_specs=[*(whole(s) for s in shapes)],
        out_shape=grads,
        scratch_shapes=sums,
        compiler_params=params,
        cost_estimate=pl.CostEstimate(flops=6 * flops, bytes_accessed=16 * tokens * hidden, transcendentals=0),
        name="second",
    )(x, dy, *w, gate, up, h, dg, du)

    chains = chains_of(range(layers), shapes, n)
    flat = [c for c in chains if c[1] < 2]
    tall = [c for c in chains if c[1] == 2]
    vmem, hbm = pl.BlockSpec(memory_space=pltpu.VMEM), pl.BlockSpec(memory_space=pl.ANY)
    blocks = [(layers, s[0] // n, s[1]) for s in shapes]
    dma = pltpu.SemaphoreType.DMA
    return pl.pallas_call(
        functools.partial(tail_kernel, n, float(sum(layers * a * b for a, b in shapes)), chains),
        in_specs=[vmem] * 6 + [hbm] * 3 + [vmem] * 6,
        out_specs=[vmem] * 9,
        out_shape=[jax.ShapeDtypeStruct(t.shape, BF16) for t in w] + [jax.ShapeDtypeStruct(b, F32) for b in blocks * 2],
        scratch_shapes=[
            pltpu.VMEM((len(flat), n - 1, max(c[5] for c in flat), hidden), BF16),
            pltpu.VMEM((len(tall), n - 1, max(c[5] for c in tall), width), BF16),
            *(pltpu.VMEM(b, BF16) for b in blocks * 2),
            pltpu.VMEM((8, 128), F32),
            pltpu.VMEM((n, 8, 128), F32),
            dma((len(chains), n - 1)), dma((len(chains), n - 1)), dma((len(chains), n - 1)), dma((len(chains), n - 1)),
            dma((n - 1,)), dma((n - 1,)), dma((3,)),
        ],
        compiler_params=pltpu.CompilerParams(collective_id=0, has_side_effects=True, vmem_limit_bytes=VMEM_LIMIT),
        name="tail",
    )(*early, *late, *w, *m, *v)


def solution(mesh):
    n = mesh.shape["dp"]
    part = P(None, "dp", None)
    whole, split = P("rep", None, None), P("rep", "dp", None)
    return jax.shard_map(
        functools.partial(on_a_device, n),
        mesh=mesh,
        in_specs=(P(("rep", "dp")), P(("rep", "dp")), P(), P(), P(), *([part] * 6)),
        out_specs=(whole,) * 3 + (split,) * 6,
        check_vma=False,
    )
```
